8 devices in a mesh: part: 1 (over z), loc: 2 (over y), grp: 4 (over x, core).
Axes of the slice: x: 2, y: 2, z: 1, core: 2. Of those that a mesh axis runs over, the one named last changes fastest.
Arguments:
- x_rows: bfloat16 [1536, 1024], P(('part', 'grp', 'loc'))
- dy_rows: bfloat16 [1536, 1024], P(('part', 'grp', 'loc'))
- expert_ids: int32 [1536, 8], P(('part', 'grp', 'loc'))
- gate_vals: float32 [1536, 8], P(('part', 'grp', 'loc'))
- w_gate: bfloat16 [128, 1024, 384], P(('part', 'grp', 'loc'))
- w_up: bfloat16 [128, 1024, 384], P(('part', 'grp', 'loc'))
- w_down: bfloat16 [128, 384, 1024], P(('part', 'grp', 'loc'))
Outputs:
- output 1: bfloat16 [1536, 1024], P(('part', 'grp', 'loc'))
- output 2: float32 [1536, 8], P(('part', 'grp', 'loc'))
- output 3: bfloat16 [128, 1024, 384], P(('part', 'grp', 'loc'))
- output 4: bfloat16 [128, 1024, 384], P(('part', 'grp', 'loc'))
- output 5: bfloat16 [128, 384, 1024], P(('part', 'grp', 'loc'))
All inputs are finite; a program needn't handle non-finite values.
Results may differ from the reference program's by a relative error of at most 0.001.
Values are sent between devices in bfloat16 or wider.
A program may use at most 1 GiB of HBM per device.

```python
import jax
import jax.numpy as jnp
from jax import lax

GROUPS = 4
LOC_DEVS = 2
TOK_DEV = 192
EXPERTS = 128
TOP_K = 8
D_MODEL = 1024
D_FF = 384

DEV_COUNT = GROUPS * LOC_DEVS
TOKENS = TOK_DEV * DEV_COUNT
NUM_ITEMS = TOKENS * TOP_K
GROUP_LIMIT = min(TOP_K // 2, GROUPS)
PER_GROUP = TOP_K // GROUP_LIMIT
GROUP_EXPERTS = EXPERTS // GROUPS
GROUP_ROWS = GROUP_LIMIT * TOK_DEV // GROUPS
MEAN_LOAD = TOK_DEV * TOP_K // EXPERTS
SPREAD_MAX = min(MEAN_LOAD, GROUP_ROWS - MEAN_LOAD)
EXPERT_CAP = DEV_COUNT * (MEAN_LOAD + SPREAD_MAX)


def block_routing(block_key):
    key_sig, key_off, key_perm, key_amp, key_slot = jax.random.split(block_key, 5)
    tok_perm = jax.random.permutation(key_sig, TOK_DEV)
    offsets = jax.random.permutation(key_off, GROUPS)[:GROUP_LIMIT]
    shifted = (tok_perm[:, None] + offsets[None, :]) % TOK_DEV
    group_of = shifted % GROUPS
    pair_pos = jnp.arange(GROUP_LIMIT)[None, :] * (TOK_DEV // GROUPS) + shifted // GROUPS
    local_perm = jax.vmap(lambda sub_key: jax.random.permutation(sub_key, GROUP_EXPERTS))(jax.random.split(key_perm, GROUPS))
    spread = jax.random.randint(key_amp, (GROUPS, GROUP_EXPERTS // 2), 0, SPREAD_MAX + 1)
    spread = spread.at[:, 0].set(SPREAD_MAX)
    counts = jnp.stack([MEAN_LOAD + spread, MEAN_LOAD - spread], axis=-1).reshape(GROUPS, GROUP_EXPERTS)
    cum_ends = jnp.cumsum(counts, axis=1)
    seq_pos = jnp.arange(PER_GROUP)[None, None, :] * GROUP_ROWS + pair_pos[:, :, None]
    rank_idx = jnp.sum(seq_pos[..., None] >= cum_ends[group_of][:, :, None, :], axis=-1)
    local_ids = local_perm[group_of[:, :, None], rank_idx]
    expert = (group_of[:, :, None] * GROUP_EXPERTS + local_ids).reshape(TOK_DEV, TOP_K)
    slot_keys = jax.random.randint(key_slot, (TOK_DEV, TOP_K), 0, 4096) * TOP_K + jnp.arange(TOP_K)[None, :]
    slot_order = jnp.argsort(slot_keys, axis=1)
    return jnp.take_along_axis(expert, slot_order, axis=1).astype(jnp.int32)


def draw_routing(route_key):
    blocks = jax.vmap(block_routing)(jax.random.split(route_key, DEV_COUNT))
    return blocks.reshape(TOKENS, TOP_K)


def setup_inputs(seed: int = 0, part: int = 0) -> dict:
    base_key = jax.random.fold_in(jax.random.key(seed), part)
    keys = jax.random.split(base_key, 7)
    x_rows = jax.random.normal(keys[0], (TOKENS, D_MODEL), jnp.float32).astype(jnp.bfloat16)
    dy_rows = jax.random.normal(keys[1], (TOKENS, D_MODEL), jnp.float32).astype(jnp.bfloat16)
    expert_ids = draw_routing(keys[2])
    gate_vals = jax.random.uniform(keys[3], (TOKENS, TOP_K), jnp.float32, 0.25, 1.0)
    w_gate = (jax.random.normal(keys[4], (EXPERTS, D_MODEL, D_FF), jnp.float32) * D_MODEL ** -0.5).astype(jnp.bfloat16)
    w_up = (jax.random.normal(keys[5], (EXPERTS, D_MODEL, D_FF), jnp.float32) * D_MODEL ** -0.5).astype(jnp.bfloat16)
    w_down = (jax.random.normal(keys[6], (EXPERTS, D_FF, D_MODEL), jnp.float32) * D_FF ** -0.5).astype(jnp.bfloat16)
    return {'x_rows': x_rows, 'dy_rows': dy_rows, 'expert_ids': expert_ids, 'gate_vals': gate_vals, 'w_gate': w_gate, 'w_up': w_up, 'w_down': w_down}


def expert_lists(expert_ids):
    flat_ids = expert_ids.reshape(-1)
    item_order = jnp.argsort(flat_ids, stable=True)
    sorted_ids = flat_ids[item_order]
    load_sizes = jnp.zeros((EXPERTS,), jnp.int32).at[flat_ids].add(1)
    starts = jnp.cumsum(load_sizes) - load_sizes
    slot_rank = jnp.arange(NUM_ITEMS) - starts[sorted_ids]
    slot_lists = jnp.full((EXPERTS * EXPERT_CAP,), NUM_ITEMS, jnp.int32)
    slot_lists = slot_lists.at[sorted_ids * EXPERT_CAP + slot_rank].set(item_order.astype(jnp.int32))
    return slot_lists.reshape(GROUPS, GROUP_EXPERTS, EXPERT_CAP)


def reference(x_rows, dy_rows, expert_ids, gate_vals, w_gate, w_up, w_down):
    slot_lists = expert_lists(expert_ids)
    gate_flat = gate_vals.reshape(-1)

    def expert_step(part_sum, inputs):
        slot_items, wg_one, wu_one, wd_one = inputs
        is_live = slot_items < NUM_ITEMS
        tok_idx = jnp.where(is_live, slot_items // TOP_K, 0)
        x_sel = jnp.where(is_live[:, None], x_rows[tok_idx], 0).astype(jnp.bfloat16)
        dy_sel = jnp.where(is_live[:, None], dy_rows[tok_idx], 0).astype(jnp.bfloat16)
        gate_sel = jnp.where(is_live, gate_flat[jnp.minimum(slot_items, NUM_ITEMS - 1)], 0.0)
        pre_gate = jnp.dot(x_sel, wg_one, preferred_element_type=jnp.float32)
        pre_up = jnp.dot(x_sel, wu_one, preferred_element_type=jnp.float32)
        sig_gate = jax.nn.sigmoid(pre_gate)
        silu_out = pre_gate * sig_gate
        hidden = (silu_out * pre_up).astype(jnp.bfloat16)
        expert_out = jnp.dot(hidden, wd_one, preferred_element_type=jnp.float32)
        dgate_sel = jnp.sum(dy_sel.astype(jnp.float32) * expert_out, axis=-1)
        d_out = (gate_sel[:, None] * dy_sel.astype(jnp.float32)).astype(jnp.bfloat16)
        d_hidden = jnp.dot(d_out, wd_one.T, preferred_element_type=jnp.float32)
        dwd_one = jnp.dot(hidden.T, d_out, preferred_element_type=jnp.float32).astype(jnp.bfloat16)
        d_pre_up = (d_hidden * silu_out).astype(jnp.bfloat16)
        d_pre_gate = (d_hidden * pre_up * sig_gate * (1.0 + pre_gate * (1.0 - sig_gate))).astype(jnp.bfloat16)
        dwg_one = jnp.dot(x_sel.T, d_pre_gate, preferred_element_type=jnp.float32).astype(jnp.bfloat16)
        dwu_one = jnp.dot(x_sel.T, d_pre_up, preferred_element_type=jnp.float32).astype(jnp.bfloat16)
        d_rows = (jnp.dot(d_pre_gate, wg_one.T, preferred_element_type=jnp.float32) + jnp.dot(d_pre_up, wu_one.T, preferred_element_type=jnp.float32)).astype(jnp.bfloat16)
        part_sum = part_sum.at[tok_idx].add(d_rows.astype(jnp.float32))
        return part_sum, (dwg_one, dwu_one, dwd_one, dgate_sel)

    def group_step(dx_acc, inputs):
        part_sum, outputs = lax.scan(expert_step, jnp.zeros((TOKENS, D_MODEL), jnp.float32), inputs)
        return dx_acc + part_sum.astype(jnp.bfloat16).astype(jnp.float32), outputs

    weights = (w_gate.reshape(GROUPS, GROUP_EXPERTS, D_MODEL, D_FF), w_up.reshape(GROUPS, GROUP_EXPERTS, D_MODEL, D_FF), w_down.reshape(GROUPS, GROUP_EXPERTS, D_FF, D_MODEL))
    dx_acc, outputs = lax.scan(group_step, jnp.zeros((TOKENS, D_MODEL), jnp.float32), (slot_lists,) + weights)
    dw_gate, dw_up, dw_down, dgate_vals = outputs
    d_gates = jnp.zeros((NUM_ITEMS + 1,), jnp.float32).at[slot_lists.reshape(-1)].set(dgate_vals.reshape(-1))
    return (dx_acc.astype(jnp.bfloat16), d_gates[:NUM_ITEMS].reshape(TOKENS, TOP_K), dw_gate.reshape(EXPERTS, D_MODEL, D_FF), dw_up.reshape(EXPERTS, D_MODEL, D_FF), dw_down.reshape(EXPERTS, D_FF, D_MODEL))
```

```python
import functools

import jax
import jax.numpy as jnp
from jax import lax
from jax.experimental import pallas as pl
from jax.experimental.pallas import tpu as pltpu
from jax.sharding import PartitionSpec as P

N_DEV = 8
N_TOK = 192
D = 1024
F = 384
TOP_K = 8
LOC_E = 16
CAP = 24
SLOTS = N_DEV * CAP
PAIR = 2 * CAP
PAIR_ROWS = LOC_E * PAIR
MESH = pl.DeviceIdType.MESH
F32 = jnp.float32
BF16 = jnp.bfloat16
ANY = pl.BlockSpec(memory_space=pl.ANY)
VMEM = pl.BlockSpec(memory_space=pltpu.VMEM)


def dev_id(g, l):
    return {'grp': g, 'loc': l}


def index_of(g, l):
    return g * 2 + l


def coords():
    g = lax.axis_index('grp')
    l = lax.axis_index('loc')
    core = lax.rem(g, 2)
    gp = g + 1 - 2 * core
    gx = lax.rem(g + 2, 4)
    gxp = lax.rem(gp + 2, 4)
    ly = 1 - l
    return g, l, gp, gx, gxp, ly


def all_barrier(g, l):
    barrier = pltpu.get_barrier_semaphore()
    for k in range(1, N_DEV):
        pl.semaphore_signal(barrier, inc=1, device_id=dev_id(lax.rem(g + k // 2, 4), lax.rem(l + k % 2, 2)), device_id_type=MESH)
    pl.semaphore_wait(barrier, N_DEV - 1)


def gather_kernel(x_ref, dy_ref, meta_ref, xa_ref, dya_ref, ma_ref, send_sem, recv_sem, meta_send, meta_recv, own_sem):
    g, l, gp, gx, gxp, ly = coords()
    me = index_of(g, l)
    role_dev = [me, index_of(gx, l), index_of(g, ly), index_of(gx, ly),
                index_of(gp, l), index_of(gxp, l), index_of(gp, ly), index_of(gxp, ly)]
    to_x, to_y, to_p = dev_id(gx, l), dev_id(g, ly), dev_id(gp, l)
    n_chunk = 4
    half = N_TOK // 2

    def piece(k, src_dev):
        ref = xa_ref if k < 2 else dya_ref
        return ref.at[src_dev, pl.ds((k % 2) * half, half)]

    def own_piece(k):
        ref = x_ref if k < 2 else dy_ref
        return ref.at[pl.ds((k % 2) * half, half)]

    sends = []

    def send(k, src_role, dst_role, target):
        src = own_piece(k) if src_role == 0 else piece(k, role_dev[src_role])
        copy = pltpu.make_async_remote_copy(
            src_ref=src, dst_ref=piece(k, role_dev[src_role]), send_sem=send_sem.at[len(sends)],
            recv_sem=recv_sem.at[dst_role, k], device_id=target, device_id_type=MESH)
        copy.start()
        sends.append(copy)

    def wait_role(role, k):
        pltpu.make_async_remote_copy(
            src_ref=own_piece(k), dst_ref=piece(k, role_dev[role]), send_sem=send_sem.at[0],
            recv_sem=recv_sem.at[role, k], device_id=to_p, device_id_type=MESH).wait_recv()

    own = [pltpu.make_async_copy(x_ref, xa_ref.at[me], own_sem.at[0]),
           pltpu.make_async_copy(dy_ref, dya_ref.at[me], own_sem.at[1]),
           pltpu.make_async_copy(meta_ref, ma_ref.at[me], own_sem.at[2])]
    for copy in own:
        copy.start()
    all_barrier(g, l)
    metas = []
    for i in range(1, N_DEV):
        tg, tl = lax.rem(g + i // 2, 4), lax.rem(l + i % 2, 2)
        copy = pltpu.make_async_remote_copy(
            src_ref=meta_ref, dst_ref=ma_ref.at[me], send_sem=meta_send.at[i], recv_sem=meta_recv.at[i],
            device_id=dev_id(tg, tl), device_id_type=MESH)
        copy.start()
        metas.append(copy)
    for k in range(n_chunk):
        send(k, 0, 1, to_x)
        send(k, 0, 2, to_y)
        send(k, 0, 4, to_p)
    for k in range(n_chunk):
        wait_role(1, k)
        if k % 2 == 0:
            send(k, 1, 3, to_y)
        send(k, 1, 5, to_p)
        wait_role(2, k)
        if k % 2 == 1:
            send(k, 2, 3, to_x)
        send(k, 2, 6, to_p)
    for k in range(n_chunk):
        wait_role(3, k)
        send(k, 3, 7, to_p)
    for k in range(n_chunk):
        for role in range(4, 8):
            wait_role(role, k)
    for i in range(1, N_DEV):
        sg, sl = lax.rem(g + 4 - i // 2, 4), lax.rem(l + i % 2, 2)
        pltpu.make_async_remote_copy(
            src_ref=meta_ref, dst_ref=ma_ref.at[index_of(sg, sl)], send_sem=meta_send.at[i], recv_sem=meta_recv.at[i],
            device_id=dev_id(sg, sl), device_id_type=MESH).wait_recv()
    for copy in metas + sends:
        copy.wait_send()
    for copy in own:
        copy.wait()


def dispatch(x_rows, dy_rows, meta):
    return pl.pallas_call(
        gather_kernel,
        out_shape=[jax.ShapeDtypeStruct((N_DEV, N_TOK, D), BF16), jax.ShapeDtypeStruct((N_DEV, N_TOK, D), BF16),
                   jax.ShapeDtypeStruct((N_DEV, 2 * TOP_K, N_TOK), F32)],
        in_specs=[ANY] * 3, out_specs=[ANY] * 3,
        scratch_shapes=[pltpu.SemaphoreType.DMA((28,)), pltpu.SemaphoreType.DMA((8, 4)), pltpu.SemaphoreType.DMA((8,)),
                        pltpu.SemaphoreType.DMA((8,)), pltpu.SemaphoreType.DMA((3,))],
        compiler_params=pltpu.CompilerParams(collective_id=0, has_side_effects=True),
        name='dispatch',
    )(x_rows, dy_rows, meta)


def dot(a, b, ca=1, cb=0):
    return lax.dot_general(a, b, (((ca,), (cb,)), ((), ())), preferred_element_type=F32)


def slot_iota(rows):
    return lax.broadcasted_iota(jnp.int32, (LOC_E, rows, N_TOK), 1).astype(F32)


def expert_kernel(xa_ref, dya_ref, ma_ref, wg_ref, wu_ref, wd_ref, dwg_ref, dwu_ref, dwd_ref, part_ref, dgate_ref,
                  xs, uds, cs, rank_s, dgs):
    e = pl.program_id(0)

    @pl.when(e == 0)
    def _():
        base = (index_of(lax.axis_index('grp'), lax.axis_index('loc')) * LOC_E).astype(F32)
        e_iota = lax.broadcasted_iota(jnp.int32, (LOC_E, N_TOK), 0).astype(F32) + base
        before = (lax.broadcasted_iota(jnp.int32, (N_TOK, N_TOK), 0) < lax.broadcasted_iota(jnp.int32, (N_TOK, N_TOK), 1)).astype(BF16)

        @pl.loop(0, N_DEV // 2)
        def _(p):
            row0 = pl.multiple_of(p * PAIR, 16)
            hots, gcols = [], []
            for h in range(2):
                d = p * 2 + h
                member = jnp.zeros((LOC_E, N_TOK), F32)
                gate = jnp.zeros((LOC_E, N_TOK), F32)
                for j in range(TOP_K):
                    hit = ma_ref[d, pl.ds(j, 1), :] == e_iota
                    member = jnp.where(hit, 1.0, member)
                    gate = jnp.where(hit, ma_ref[d, pl.ds(TOP_K + j, 1), :], gate)
                rank = jnp.where(member > 0, dot(member.astype(BF16), before), -1000.0)
                rank_s[d] = rank
                mask = rank[:, None, :] == slot_iota(CAP)
                gcols.append(jnp.sum(jnp.where(mask, gate[:, None, :], 0.0), axis=2, keepdims=True))
                hots.append(jnp.where(mask, 1.0, 0.0).reshape(LOC_E * CAP, N_TOK).astype(BF16))
            gcol = jnp.concatenate(gcols, axis=1)
            for c in range(4):
                cols = slice(c * 256, (c + 1) * 256)
                xv = jnp.concatenate([dot(hots[h], xa_ref[p * 2 + h, :, cols]).reshape(LOC_E, CAP, 256) for h in range(2)], axis=1)
                xs[:, pl.ds(row0, PAIR), cols] = xv.astype(BF16)
                yv = jnp.concatenate([dot(hots[h], dya_ref[p * 2 + h, :, cols]).reshape(LOC_E, CAP, 256) for h in range(2)], axis=1)
                uds[:, pl.ds(row0, PAIR), cols] = (gcol * yv).astype(BF16)
                uds[:, pl.ds(pl.multiple_of(row0 + SLOTS, 16), PAIR), cols] = yv.astype(BF16)

    x = xs[e]
    pre_gate = dot(x, wg_ref[0])
    pre_up = dot(x, wu_ref[0])
    sig = jax.nn.sigmoid(pre_gate)
    silu = pre_gate * sig
    hidden = (silu * pre_up).astype(BF16)
    back = dot(uds[e], wd_ref[0], 1, 1)
    d_hidden = back[:SLOTS]
    dgs[e] = jnp.broadcast_to(jnp.sum(hidden.astype(F32) * back[SLOTS:], axis=1, keepdims=True), (SLOTS, 128))
    d_up = (d_hidden * silu).astype(BF16)
    d_gate = (d_hidden * pre_up * sig * (1.0 + pre_gate * (1.0 - sig))).astype(BF16)
    c = (dot(d_gate, wg_ref[0], 1, 1) + dot(d_up, wu_ref[0], 1, 1)).astype(BF16)
    for p in range(N_DEV // 2):
        cs[p, pl.ds(pl.multiple_of(e * PAIR, 16), PAIR), :] = c[p * PAIR:(p + 1) * PAIR]
    dwd_ref[0] = dot(hidden, uds[e, :SLOTS], 0, 0).astype(BF16)
    dwg_ref[0] = dot(x, d_gate, 0, 0).astype(BF16)
    dwu_ref[0] = dot(x, d_up, 0, 0).astype(BF16)

    @pl.when(e == LOC_E - 1)
    def _():
        @pl.loop(0, N_DEV // 2)
        def _(p):
            for h in range(2):
                d = p * 2 + h
                rank = rank_s[d]
                mask = rank[:, None, :] == slot_iota(CAP)
                vals = dgs[:, pl.ds(pl.multiple_of(p * PAIR + h * CAP, 8), CAP), :][:, :, :1]
                dgate_ref[d] = jnp.sum(jnp.where(mask, vals, 0.0), axis=1)
                wide = (rank + float(h * CAP))[:, None, :] == slot_iota(PAIR)
                hot = jnp.where(wide, 1.0, 0.0).reshape(PAIR_ROWS, N_TOK).astype(BF16)
                for q in range(4):
                    cols = slice(q * 256, (q + 1) * 256)
                    part_ref[d, :, cols] = dot(hot, cs[p, :, cols], 0, 0).astype(BF16)


def expert_stage(xa, dya, meta_all, w_gate, w_up, w_down):
    whole = lambda *shape: pl.BlockSpec(shape, lambda e: (0,) * len(shape), pipeline_mode=pl.Buffered(1))
    each = lambda *shape: pl.BlockSpec((1,) + shape, lambda e: (e, 0, 0))
    return pl.pallas_call(
        expert_kernel,
        grid=(LOC_E,),
        out_shape=[jax.ShapeDtypeStruct((LOC_E, D, F), BF16), jax.ShapeDtypeStruct((LOC_E, D, F), BF16), jax.ShapeDtypeStruct((LOC_E, F, D), BF16),
                   jax.ShapeDtypeStruct((N_DEV, N_TOK, D), BF16), jax.ShapeDtypeStruct((N_DEV, LOC_E, N_TOK), F32)],
        in_specs=[whole(N_DEV, N_TOK, D), whole(N_DEV, N_TOK, D), whole(N_DEV, 2 * TOP_K, N_TOK), each(D, F), each(D, F), each(F, D)],
        out_specs=[each(D, F), each(D, F), each(F, D), whole(N_DEV, N_TOK, D), whole(N_DEV, LOC_E, N_TOK)],
        scratch_shapes=[pltpu.VMEM((LOC_E, SLOTS, D), BF16), pltpu.VMEM((LOC_E, 2 * SLOTS, D), BF16), pltpu.VMEM((N_DEV // 2, PAIR_ROWS, D), BF16),
                        pltpu.VMEM((N_DEV, LOC_E, N_TOK), F32), pltpu.VMEM((LOC_E, SLOTS, 128), F32)],
        compiler_params=pltpu.CompilerParams(vmem_limit_bytes=60 * 1024 * 1024, dimension_semantics=('arbitrary',)),
        name='experts',
    )(xa, dya, meta_all, w_gate, w_up, w_down)


def combine_kernel(part_ref, dgate_ref, ids_ref, dx_ref, dg_ref, pv, dv, send_sem, recv_sem, own_sem):
    g = lax.axis_index('grp')
    l = lax.axis_index('loc')
    me = index_of(g, l)
    own = [pltpu.make_async_copy(part_ref.at[me], pv.at[me], own_sem.at[0]), pltpu.make_async_copy(dgate_ref.at[me], dv.at[me], own_sem.at[1])]
    for copy in own:
        copy.start()
    all_barrier(g, l)
    sends = []
    for i in range(1, N_DEV):
        tg, tl = lax.rem(g + i // 2, 4), lax.rem(l + i % 2, 2)
        them = index_of(tg, tl)
        for a, (src, dst) in enumerate(((dgate_ref, dv), (part_ref, pv))):
            copy = pltpu.make_async_remote_copy(
                src_ref=src.at[them], dst_ref=dst.at[me], send_sem=send_sem.at[i, a], recv_sem=recv_sem.at[i, a],
                device_id=dev_id(tg, tl), device_id_type=MESH)
            copy.start()
            sends.append(copy)
    for i in range(1, N_DEV):
        sg, sl = lax.rem(g + 4 - i // 2, 4), lax.rem(l + i % 2, 2)
        them = index_of(sg, sl)
        for a, (src, dst) in enumerate(((dgate_ref, dv), (part_ref, pv))):
            pltpu.make_async_remote_copy(
                src_ref=src.at[them], dst_ref=dst.at[them], send_sem=send_sem.at[i, a], recv_sem=recv_sem.at[i, a],
                device_id=dev_id(sg, sl), device_id_type=MESH).wait_recv()
    for copy in own:
        copy.wait()
    for copy in sends:
        copy.wait_send()

    @pl.loop(0, N_TOK // 16)
    def _(r):
        rows = pl.ds(pl.multiple_of(r * 16, 16), 16)
        total = jnp.zeros((16, D), F32)
        for q in range(N_DEV // 2):
            total += (pv[2 * q, rows].astype(F32) + pv[2 * q + 1, rows].astype(F32)).astype(BF16).astype(F32)
        dx_ref[rows] = total.astype(BF16)

    e_iota = lax.broadcasted_iota(jnp.int32, (LOC_E, N_TOK), 0)
    for j in range(TOP_K):
        want = ids_ref[pl.ds(j, 1), :]
        acc = jnp.zeros((LOC_E, N_TOK), F32)
        for d in range(N_DEV):
            acc = jnp.where(want == e_iota + d * LOC_E, dv[d], acc)
        dg_ref[pl.ds(j, 1), :] = jnp.sum(acc, axis=0, keepdims=True)


def combine(part, dgate, ids_t):
    return pl.pallas_call(
        combine_kernel,
        out_shape=[jax.ShapeDtypeStruct((N_TOK, D), BF16), jax.ShapeDtypeStruct((TOP_K, N_TOK), F32)],
        in_specs=[ANY, ANY, VMEM], out_specs=[VMEM, VMEM],
        scratch_shapes=[pltpu.VMEM((N_DEV, N_TOK, D), BF16), pltpu.VMEM((N_DEV, LOC_E, N_TOK), F32),
                        pltpu.SemaphoreType.DMA((8, 2)), pltpu.SemaphoreType.DMA((8, 2)), pltpu.SemaphoreType.DMA((2,))],
        compiler_params=pltpu.CompilerParams(collective_id=1, has_side_effects=True, vmem_limit_bytes=32 * 1024 * 1024),
        name='combine',
    )(part, dgate, ids_t)


def solution(mesh):
    spec = P(('part', 'grp', 'loc'))

    def device_step(x_rows, dy_rows, expert_ids, gate_vals, w_gate, w_up, w_down):
        ids_t = expert_ids.T
        meta = jnp.concatenate([ids_t.astype(F32), gate_vals.T], axis=0)
        xa, dya, meta_all = dispatch(x_rows, dy_rows, meta)
        dwg, dwu, dwd, part, dgate = expert_stage(xa, dya, meta_all, w_gate, w_up, w_down)
        dx, dg_t = combine(part, dgate, ids_t)
        return dx, dg_t.T, dwg, dwu, dwd

    return jax.shard_map(device_step, mesh=mesh, in_specs=(spec,) * 7, out_specs=(spec,) * 5, check_vma=False)
```

```python
import jax
import jax.numpy as jnp
from jax import lax
from jax.experimental import pallas as pl
from jax.experimental.pallas import tpu as pltpu
from jax.sharding import PartitionSpec as P

N_DEV = 8
N_TOK = 192
HALF = N_TOK // 2
D = 1024
F = 384
TOP_K = 8
LOC_E = 16
CAP = 24
SLOTS = N_DEV * CAP
PAIR = 2 * CAP
PAIR_ROWS = LOC_E * PAIR
N_PAIR = N_DEV // 2
RING = 4
MESH = pl.DeviceIdType.MESH
F32 = jnp.float32
BF16 = jnp.bfloat16
ANY = pl.BlockSpec(memory_space=pl.ANY)
VMEM = pl.BlockSpec(memory_space=pltpu.VMEM)


def dot(a, b, ca=1, cb=0):
    return lax.dot_general(a, b, (((ca,), (cb,)), ((), ())), preferred_element_type=F32)


def role_coords(role):
    g = lax.axis_index('grp')
    l = lax.axis_index('loc')
    if role & 1:
        g = g + 1 - 2 * lax.rem(g, 2)
    if role & 2:
        g = lax.rem(g + 2, 4)
    if role & 4:
        l = 1 - l
    return g, l


def role_id(role):
    g, l = role_coords(role)
    return {'grp': g, 'loc': l}


def role_expert_base(role):
    g, l = role_coords(role)
    return (g * 2 + l) * LOC_E


def slot_iota(rows):
    return lax.broadcasted_iota(jnp.int32, (LOC_E, rows, N_TOK), 1).astype(F32)


def front_kernel(x_ref, dy_ref, meta_ref, wg_ref, wu_ref, wd_ref,
                 part_ref, dgate_ref, xs_ref, us_ref, hid_ref, dab_ref,
                 xa, dya, ma, xs, uds, cs, hots, gcols, ranks, back, dgs, wd_buf, w_buf, hid_st, dab_st, dg_out, dg_in, part_st,
                 send_sem, recv_sem, meta_send, meta_recv, dg_send, dg_recv, own_sem, wd_sem, w_sem, st_sem, out_sem):
    P_, X_, Y_ = 1, 2, 4
    data = (dya, xa)
    raw = (dy_ref, x_ref)
    sends = []

    def piece(a, role, k):
        return data[a].at[role, pl.ds(k * HALF, HALF)]

    def send(a, k, src_role, hop):
        dst_role = src_role ^ hop
        src = raw[a].at[pl.ds(k * HALF, HALF)] if src_role == 0 else piece(a, src_role, k)
        copy = pltpu.make_async_remote_copy(
            src_ref=src, dst_ref=piece(a, dst_role, k), send_sem=send_sem.at[len(sends)],
            recv_sem=recv_sem.at[a, dst_role, k], device_id=role_id(hop), device_id_type=MESH)
        copy.start()
        sends.append(copy)

    def arrived(a, role, k):
        pltpu.make_async_remote_copy(
            src_ref=piece(a, role, k), dst_ref=piece(a, role, k), send_sem=send_sem.at[0],
            recv_sem=recv_sem.at[a, role, k], device_id=role_id(P_), device_id_type=MESH).wait_recv()

    def wd_copy(e):
        slot = lax.rem(e, RING)
        return pltpu.make_async_copy(wd_ref.at[e], wd_buf.at[slot], wd_sem.at[slot])

    def w_copies(e):
        slot = lax.rem(e, RING)
        return (pltpu.make_async_copy(wg_ref.at[e], w_buf.at[slot, :, pl.ds(0, F)], w_sem.at[slot, 0]),
                pltpu.make_async_copy(wu_ref.at[e], w_buf.at[slot, :, pl.ds(F, F)], w_sem.at[slot, 1]))

    own = [pltpu.make_async_copy(meta_ref, ma.at[0], own_sem.at[0]), pltpu.make_async_copy(dy_ref, dya.at[0], own_sem.at[1]),
           pltpu.make_async_copy(x_ref, xa.at[0], own_sem.at[2])]
    for copy in own:
        copy.start()
    for e in range(RING):
        wd_copy(e).start()
    for e in range(RING):
        for copy in w_copies(e):
            copy.start()

    barrier = pltpu.get_barrier_semaphore()
    for role in range(1, N_DEV):
        pl.semaphore_signal(barrier, inc=1, device_id=role_id(role), device_id_type=MESH)
    pl.semaphore_wait(barrier, N_DEV - 1)

    metas = []
    for role in range(1, N_DEV):
        copy = pltpu.make_async_remote_copy(
            src_ref=meta_ref, dst_ref=ma.at[role], send_sem=meta_send.at[role], recv_sem=meta_recv.at[role],
            device_id=role_id(role), device_id_type=MESH)
        copy.start()
        metas.append(copy)
    for k in range(2):
        send(0, k, 0, X_)
        send(0, 1 - k, 0, Y_)
        send(0, k, 0, P_)
    own[0].wait()
    for copy in metas:
        copy.wait_recv()

    e_iota = (lax.broadcasted_iota(jnp.int32, (LOC_E, N_TOK), 0) + role_expert_base(0)).astype(F32)
    before = (lax.broadcasted_iota(jnp.int32, (N_TOK, N_TOK), 0) < lax.broadcasted_iota(jnp.int32, (N_TOK, N_TOK), 1)).astype(BF16)

    @pl.loop(0, N_DEV)
    def _(r):
        member = jnp.zeros((LOC_E, N_TOK), F32)
        gate = jnp.zeros((LOC_E, N_TOK), F32)
        meta = ma[r]
        for j in range(TOP_K):
            hit = meta[j:j + 1] == e_iota
            member = jnp.where(hit, 1.0, member)
            gate = jnp.where(hit, meta[TOP_K + j:TOP_K + j + 1], gate)
        rank = jnp.where(member > 0, dot(member.astype(BF16), before), -1000.0)
        ranks[r] = rank
        mask = rank[:, None, :] == slot_iota(CAP)
        gcol = jnp.sum(jnp.where(mask, gate[:, None, :], 0.0), axis=2, keepdims=True)
        gcols[r] = jnp.broadcast_to(gcol, (LOC_E, CAP, 128))
        hots[r] = jnp.where(mask, 1.0, 0.0).reshape(LOC_E * CAP, N_TOK).astype(BF16)

    def gather(a, q):
        @pl.loop(0, 4)
        def _(c):
            cols = pl.ds(pl.multiple_of(c * 256, 256), 256)
            rows = pl.ds(q * PAIR, PAIR)
            vals = jnp.concatenate([dot(hots[2 * q + h], data[a][2 * q + h, :, cols]).reshape(LOC_E, CAP, 256) for h in range(2)], axis=1)
            if a == 1:
                xs[:, rows, cols] = vals.astype(BF16)
            else:
                gcol = jnp.concatenate([gcols[2 * q + h][:, :, :1] for h in range(2)], axis=1)
                uds[:, rows, cols] = (gcol * vals).astype(BF16)
                uds[:, pl.ds(SLOTS + q * PAIR, PAIR), cols] = vals.astype(BF16)

    def first_relays(a):
        arrived(a, X_, 0)
        send(a, 0, X_, Y_)
        send(a, 0, X_, P_)
        arrived(a, Y_, 1)
        send(a, 1, Y_, X_)
        send(a, 1, Y_, P_)

    def second_forwards(a):
        arrived(a, X_, 1)
        send(a, 1, X_, P_)
        arrived(a, Y_, 0)
        send(a, 0, Y_, P_)

    def last_forwards(a):
        for k in range(2):
            arrived(a, X_ | Y_, k)
            send(a, k, X_ | Y_, P_)

    own[1].wait()
    for k in range(2):
        arrived(0, P_, k)
    gather(0, 0)
    first_relays(0)
    for k in range(2):
        send(1, k, 0, X_)
        send(1, 1 - k, 0, Y_)
        send(1, k, 0, P_)
    own[2].wait()
    second_forwards(0)
    for role in (X_ | P_, Y_ | P_):
        for k in range(2):
            arrived(0, role, k)
    gather(0, 1)
    gather(0, 2)
    for k in range(2):
        arrived(1, P_, k)
    gather(1, 0)
    last_forwards(0)
    for k in range(2):
        arrived(0, X_ | Y_ | P_, k)
    gather(0, 3)
    us_copy = pltpu.make_async_copy(uds.at[:, pl.ds(0, SLOTS)], us_ref, out_sem.at[0])
    us_copy.start()

    def back_step(e):
        slot = lax.rem(e, RING)
        wd_copy(e).wait()
        back[e] = dot(uds[e], wd_buf[slot], 1, 1)

        @pl.when(e + RING < LOC_E)
        def _():
            wd_copy(e + RING).start()

    pl.loop(0, LOC_E // 2)(back_step)
    first_relays(1)
    pl.loop(LOC_E // 2, LOC_E)(back_step)
    second_forwards(1)
    for role in (X_ | P_, Y_ | P_):
        for k in range(2):
            arrived(1, role, k)
    gather(1, 1)
    gather(1, 2)
    last_forwards(1)
    for k in range(2):
        arrived(1, X_ | Y_ | P_, k)
    gather(1, 3)
    xs_copy = pltpu.make_async_copy(xs, xs_ref, out_sem.at[1])
    xs_copy.start()

    def st_copies(e):
        slot = lax.rem(e, 2)
        return (pltpu.make_async_copy(hid_st.at[slot], hid_ref.at[e], st_sem.at[slot, 0]),
                pltpu.make_async_copy(dab_st.at[slot], dab_ref.at[e], st_sem.at[slot, 1]))

    @pl.loop(0, LOC_E)
    def _(e):
        slot = lax.rem(e, RING)
        st = lax.rem(e, 2)
        for copy in w_copies(e):
            copy.wait()

        @pl.when(e >= 2)
        def _():
            for copy in st_copies(e - 2):
                copy.wait()

        pre = dot(xs[e], w_buf[slot])
        pre_gate = pre[:, :F]
        pre_up = pre[:, F:]
        sig = jax.nn.sigmoid(pre_gate)
        silu = pre_gate * sig
        hidden = (silu * pre_up).astype(BF16)
        d_hidden = back[e, :SLOTS]
        dgs[e] = jnp.broadcast_to(jnp.sum(hidden.astype(F32) * back[e, SLOTS:], axis=1, keepdims=True), (SLOTS, 128))
        d_up = (d_hidden * silu).astype(BF16)
        d_gate = (d_hidden * pre_up * sig * (1.0 + pre_gate * (1.0 - sig))).astype(BF16)
        hid_st[st] = hidden
        dab = jnp.concatenate([d_gate, d_up], axis=1)
        dab_st[st] = dab
        for copy in st_copies(e):
            copy.start()
        c = dot(dab, w_buf[slot], 1, 1).astype(BF16)
        for q in range(N_PAIR):
            cs[q, pl.ds(pl.multiple_of(e * PAIR, 16), PAIR), :] = c[q * PAIR:(q + 1) * PAIR]

        @pl.when(e + RING < LOC_E)
        def _():
            for copy in w_copies(e + RING):
                copy.start()

    dg_copies = []
    for r in range(N_DEV):
        mask = ranks[r][:, None, :] == slot_iota(CAP)
        vals = dgs[:, r * CAP:(r + 1) * CAP, :][:, :, :1]
        dg_out[r] = jnp.sum(jnp.where(mask, vals, 0.0), axis=1)
        if r:
            copy = pltpu.make_async_remote_copy(
                src_ref=dg_out.at[r], dst_ref=dg_in.at[r], send_sem=dg_send.at[r], recv_sem=dg_recv.at[r],
                device_id=role_id(r), device_id_type=MESH)
            copy.start()
            dg_copies.append(copy)

    part_copies = []
    for r in range(N_DEV):
        q, h = r // 2, r % 2

        wide = (ranks[r] + float(h * CAP))[:, None, :] == slot_iota(PAIR)
        hot = jnp.where(wide, 1.0, 0.0).reshape(PAIR_ROWS, N_TOK).astype(BF16)
        for c in range(4):
            cols = slice(c * 256, (c + 1) * 256)
            part_st[r, :, cols] = dot(hot, cs[q, :, cols], 0, 0).astype(BF16)
        g, l = role_coords(r)
        copy = pltpu.make_async_copy(part_st.at[r], part_ref.at[l * 4 + g], out_sem.at[2 + r])
        copy.start()
        part_copies.append(copy)

    for copy in dg_copies:
        copy.wait_recv()
    bases = [role_expert_base(r) for r in range(N_DEV)]
    row_iota = lax.broadcasted_iota(jnp.int32, (LOC_E, N_TOK), 0)
    for j in range(TOP_K):
        want = ma[0, j:j + 1, :]
        acc = jnp.zeros((LOC_E, N_TOK), F32)
        for r in range(N_DEV):
            acc = jnp.where(want == (row_iota + bases[r]).astype(F32), dg_in[r] if r else dg_out[0], acc)
        dgate_ref[pl.ds(j, 1), :] = jnp.sum(acc, axis=0, keepdims=True)

    for e in (LOC_E - 2, LOC_E - 1):
        for copy in st_copies(e):
            copy.wait()
    for copy in [us_copy, xs_copy] + part_copies:
        copy.wait()
    for copy in sends + metas + dg_copies:
        copy.wait_send()


def front(x_rows, dy_rows, meta, w_gate, w_up, w_down):
    dma = pltpu.SemaphoreType.DMA
    return pl.pallas_call(
        front_kernel,
        out_shape=[jax.ShapeDtypeStruct((N_DEV, N_TOK, D), BF16), jax.ShapeDtypeStruct((TOP_K, N_TOK), F32),
                   jax.ShapeDtypeStruct((LOC_E, SLOTS, D), BF16), jax.ShapeDtypeStruct((LOC_E, SLOTS, D), BF16),
                   jax.ShapeDtypeStruct((LOC_E, SLOTS, F), BF16), jax.ShapeDtypeStruct((LOC_E, SLOTS, 2 * F), BF16)],
        in_specs=[ANY] * 6, out_specs=[ANY, VMEM] + [ANY] * 4,
        scratch_shapes=[
            pltpu.VMEM((N_DEV, N_TOK, D), BF16), pltpu.VMEM((N_DEV, N_TOK, D), BF16), pltpu.VMEM((N_DEV, 2 * TOP_K, N_TOK), F32),
            pltpu.VMEM((LOC_E, SLOTS, D), BF16), pltpu.VMEM((LOC_E, 2 * SLOTS, D), BF16), pltpu.VMEM((N_PAIR, PAIR_ROWS, D), BF16),
            pltpu.VMEM((N_DEV, LOC_E * CAP, N_TOK), BF16), pltpu.VMEM((N_DEV, LOC_E, CAP, 128), F32), pltpu.VMEM((N_DEV, LOC_E, N_TOK), F32),
            pltpu.VMEM((LOC_E, 2 * SLOTS, F), F32), pltpu.VMEM((LOC_E, SLOTS, 128), F32),
            pltpu.VMEM((RING, F, D), BF16), pltpu.VMEM((RING, D, 2 * F), BF16), pltpu.VMEM((2, SLOTS, F), BF16), pltpu.VMEM((2, SLOTS, 2 * F), BF16),
            pltpu.VMEM((N_DEV, LOC_E, N_TOK), F32), pltpu.VMEM((N_DEV, LOC_E, N_TOK), F32), pltpu.VMEM((N_DEV, N_TOK, D), BF16),
            dma((40,)), dma((2, N_DEV, 2)), dma((N_DEV,)), dma((N_DEV,)), dma((N_DEV,)), dma((N_DEV,)), dma((3,)),
            dma((RING,)), dma((RING, 2)), dma((2, 2)), dma((2 + N_DEV,))],
        compiler_params=pltpu.CompilerParams(collective_id=0, has_side_effects=True, vmem_limit_bytes=63 * 1024 * 1024),
        name='front',
    )(x_rows, dy_rows, meta, w_gate, w_up, w_down)


def wgrad_kernel(x_ref, u_ref, hid_ref, dab_ref, dwg_ref, dwu_ref, dwd_ref):
    dwd_ref[0] = dot(hid_ref[0], u_ref[0], 0, 0).astype(BF16)
    both = dot(x_ref[0], dab_ref[0], 0, 0).astype(BF16)
    dwg_ref[0] = both[:, :F]
    dwu_ref[0] = both[:, F:]


def wgrad(xs, us, hid, dab):
    each = lambda *shape: pl.BlockSpec((1,) + shape, lambda e: (e, 0, 0))
    return pl.pallas_call(
        wgrad_kernel,
        grid=(LOC_E,),
        out_shape=[jax.ShapeDtypeStruct((LOC_E, D, F), BF16), jax.ShapeDtypeStruct((LOC_E, D, F), BF16), jax.ShapeDtypeStruct((LOC_E, F, D), BF16)],
        in_specs=[each(SLOTS, D), each(SLOTS, D), each(SLOTS, F), each(SLOTS, 2 * F)],
        out_specs=[each(D, F), each(D, F), each(F, D)],
        compiler_params=pltpu.CompilerParams(vmem_limit_bytes=60 * 1024 * 1024, dimension_semantics=('arbitrary',)),
        cost_estimate=pl.CostEstimate(flops=2 * LOC_E * SLOTS * D * F * 3, bytes_accessed=57_000_000, transcendentals=0),
        name='wgrad',
    )(xs, us, hid, dab)


def final_kernel(parts_ref, dx_ref):
    @pl.loop(0, N_TOK // 16)
    def _(i):
        rows = pl.ds(pl.multiple_of(i * 16, 16), 16)
        total = jnp.zeros((16, D), F32)
        for g in range(4):
            total += (parts_ref[g, rows].astype(F32) + parts_ref[4 + g, rows].astype(F32)).astype(BF16).astype(F32)
        dx_ref[rows] = total.astype(BF16)


def final_sum(parts):
    return pl.pallas_call(
        final_kernel,
        out_shape=jax.ShapeDtypeStruct((N_TOK, D), BF16),
        in_specs=[VMEM],
        out_specs=VMEM,
        compiler_params=pltpu.CompilerParams(vmem_limit_bytes=16 * 1024 * 1024),
        name='final_sum',
    )(parts)


def solution(mesh):
    spec = P(('part', 'grp', 'loc'))

    def device_step(x_rows, dy_rows, expert_ids, gate_vals, w_gate, w_up, w_down):
        meta = jnp.concatenate([expert_ids.T.astype(F32), gate_vals.T], axis=0)
        part, dgate_t, xs, us, hid, dab = front(x_rows, dy_rows, meta, w_gate, w_up, w_down)
        parts = lax.all_to_all(part, ('loc', 'grp'), 0, 0)
        dwg, dwu, dwd = wgrad(xs, us, hid, dab)
        return final_sum(parts), dgate_t.T, dwg, dwu, dwd

    return jax.shard_map(device_step, mesh=mesh, in_specs=(spec,) * 7, out_specs=(spec,) * 5, check_vma=False)
```

```python
import jax
import jax.numpy as jnp
from jax import lax
from jax.experimental import pallas as pl
from jax.experimental.pallas import tpu as pltpu
from jax.sharding import PartitionSpec as P

N_DEV = 8
N_TOK = 192
HALF = N_TOK // 2
D = 1024
F = 384
TOP_K = 8
LOC_E = 16
CAP = 24
SLOTS = N_DEV * CAP
PAIR = 2 * CAP
PAIR_ROWS = LOC_E * PAIR
N_PAIR = N_DEV // 2
RING = 4
W_RING = 6
MESH = pl.DeviceIdType.MESH
F32 = jnp.float32
BF16 = jnp.bfloat16
ANY = pl.BlockSpec(memory_space=pl.ANY)
VMEM = pl.BlockSpec(memory_space=pltpu.VMEM)


def dot(a, b, ca=1, cb=0):
    return lax.dot_general(a, b, (((ca,), (cb,)), ((), ())), preferred_element_type=F32)


def role_coords(role):
    g = lax.axis_index('grp')
    l = lax.axis_index('loc')
    if role & 1:
        g = g + 1 - 2 * lax.rem(g, 2)
    if role & 2:
        g = lax.rem(g + 2, 4)
    if role & 4:
        l = 1 - l
    return g, l


def role_id(role):
    g, l = role_coords(role)
    return {'grp': g, 'loc': l}


def role_expert_base(role):
    g, l = role_coords(role)
    return (g * 2 + l) * LOC_E


def slot_iota(rows):
    return lax.broadcasted_iota(jnp.int32, (LOC_E, rows, N_TOK), 1).astype(F32)


def front_kernel(x_ref, dy_ref, ids_ref, gates_ref, wg_ref, wu_ref, wd_ref,
                 part_ref, dgate_ref, xs_ref, us_ref, hid_ref, dab_ref,
                 xa, dya, ids_all, gates_all, xs, uds, cs, hots, gcols, ranks, back, dgs, wd_buf, w_buf, pre0, pre1, hid0, hid1, dab0, dab1, dg_out, dg_in,
                 send_sem, recv_sem, ids_send, ids_recv, gates_send, gates_recv, dg_send, dg_recv, own_sem, wd_sem, w_sem, st_sem, out_sem):
    P_, X_, Y_ = 1, 2, 4
    data = (dya, xa)
    raw = (dy_ref, x_ref)
    sends = []

    def piece(a, role, k):
        return data[a].at[role, pl.ds(k * HALF, HALF)]

    def send(a, k, src_role, hop):
        dst_role = src_role ^ hop
        src = raw[a].at[pl.ds(k * HALF, HALF)] if src_role == 0 else piece(a, src_role, k)
        copy = pltpu.make_async_remote_copy(
            src_ref=src, dst_ref=piece(a, dst_role, k), send_sem=send_sem.at[len(sends)],
            recv_sem=recv_sem.at[a, dst_role, k], device_id=role_id(hop), device_id_type=MESH)
        copy.start()
        sends.append(copy)

    def arrived(a, role, k):
        pltpu.make_async_remote_copy(
            src_ref=piece(a, role, k), dst_ref=piece(a, role, k), send_sem=send_sem.at[0],
            recv_sem=recv_sem.at[a, role, k], device_id=role_id(P_), device_id_type=MESH).wait_recv()

    def wd_copy(e):
        slot = lax.rem(e, RING)
        return pltpu.make_async_copy(wd_ref.at[e], wd_buf.at[slot], wd_sem.at[slot])

    def w_copies(e):
        slot = lax.rem(e, W_RING)
        return (pltpu.make_async_copy(wg_ref.at[e], w_buf.at[slot, :, pl.ds(0, F)], w_sem.at[slot, 0]),
                pltpu.make_async_copy(wu_ref.at[e], w_buf.at[slot, :, pl.ds(F, F)], w_sem.at[slot, 1]))

    own = [pltpu.make_async_copy(ids_ref, ids_all.at[0], own_sem.at[0]), pltpu.make_async_copy(dy_ref, dya.at[0], own_sem.at[1]),
           pltpu.make_async_copy(x_ref, xa.at[0], own_sem.at[2]), pltpu.make_async_copy(gates_ref, gates_all.at[0], own_sem.at[3])]
    for copy in own:
        copy.start()
    for e in range(RING):
        wd_copy(e).start()
    for e in range(W_RING):
        for copy in w_copies(e):
            copy.start()

    barrier = pltpu.get_barrier_semaphore()
    for role in range(1, N_DEV):
        pl.semaphore_signal(barrier, inc=1, device_id=role_id(role), device_id_type=MESH)
    pl.semaphore_wait(barrier, N_DEV - 1)

    metas = []
    for role in range(1, N_DEV):
        for src, dst, send_s, recv_s in ((ids_ref, ids_all, ids_send, ids_recv), (gates_ref, gates_all, gates_send, gates_recv)):
            copy = pltpu.make_async_remote_copy(
                src_ref=src, dst_ref=dst.at[role], send_sem=send_s.at[role], recv_sem=recv_s.at[role],
                device_id=role_id(role), device_id_type=MESH)
            copy.start()
            metas.append(copy)
    for k in range(2):
        send(0, k, 0, X_)
        send(0, 1 - k, 0, Y_)
        send(0, k, 0, P_)
    own[0].wait()
    own[3].wait()
    for copy in metas:
        copy.wait_recv()

    e_iota = (lax.broadcasted_iota(jnp.int32, (LOC_E, N_TOK), 0) + role_expert_base(0))
    before = (lax.broadcasted_iota(jnp.int32, (N_TOK, N_TOK), 0) < lax.broadcasted_iota(jnp.int32, (N_TOK, N_TOK), 1)).astype(BF16)

    @pl.loop(0, N_DEV)
    def _(r):
        member = jnp.zeros((LOC_E, N_TOK), F32)
        gate = jnp.zeros((LOC_E, N_TOK), F32)
        ids = ids_all[r]
        gates = gates_all[r]
        for j in range(TOP_K):
            hit = ids[j:j + 1] == e_iota
            member = jnp.where(hit, 1.0, member)
            gate = jnp.where(hit, gates[j:j + 1], gate)
        rank = jnp.where(member > 0, dot(member.astype(BF16), before), -1000.0)
        ranks[r] = rank
        mask = rank[:, None, :] == slot_iota(CAP)
        gcol = jnp.sum(jnp.where(mask, gate[:, None, :], 0.0), axis=2, keepdims=True)
        gcols[r] = jnp.broadcast_to(gcol, (LOC_E, CAP, 128))
        hots[r] = jnp.where(mask, 1.0, 0.0).reshape(LOC_E * CAP, N_TOK).astype(BF16)

    def gather(a, q):
        @pl.loop(0, 4, unroll=4)
        def _(c):
            cols = pl.ds(pl.multiple_of(c * 256, 256), 256)
            rows = pl.ds(q * PAIR, PAIR)
            vals = jnp.concatenate([dot(hots[2 * q + h], data[a][2 * q + h, :, cols]).reshape(LOC_E, CAP, 256) for h in range(2)], axis=1)
            if a == 1:
                xs[:, rows, cols] = vals.astype(BF16)
            else:
                gcol = jnp.concatenate([gcols[2 * q + h][:, :, :1] for h in range(2)], axis=1)
                uds[:, rows, cols] = (gcol * vals).astype(BF16)
                uds[:, pl.ds(SLOTS + q * PAIR, PAIR), cols] = vals.astype(BF16)

    def first_relays(a):
        arrived(a, X_, 0)
        send(a, 0, X_, Y_)
        send(a, 0, X_, P_)
        arrived(a, Y_, 1)
        send(a, 1, Y_, X_)
        send(a, 1, Y_, P_)

    def second_forwards(a):
        arrived(a, X_, 1)
        send(a, 1, X_, P_)
        arrived(a, Y_, 0)
        send(a, 0, Y_, P_)

    def last_forwards(a):
        for k in range(2):
            arrived(a, X_ | Y_, k)
            send(a, k, X_ | Y_, P_)

    own[1].wait()
    for k in range(2):
        arrived(0, P_, k)
    gather(0, 0)
    first_relays(0)
    for k in range(2):
        send(1, k, 0, X_)
        send(1, 1 - k, 0, Y_)
        send(1, k, 0, P_)
    own[2].wait()
    second_forwards(0)
    for role in (X_ | P_, Y_ | P_):
        for k in range(2):
            arrived(0, role, k)
    gather(0, 1)
    gather(0, 2)
    for k in range(2):
        arrived(1, P_, k)
    gather(1, 0)
    last_forwards(0)
    for k in range(2):
        arrived(0, X_ | Y_ | P_, k)
    gather(0, 3)
    us_copy = pltpu.make_async_copy(uds.at[:, pl.ds(0, SLOTS)], us_ref, out_sem.at[0])
    us_copy.start()

    def back_step(e):
        slot = lax.rem(e, RING)
        wd_copy(e).wait()
        back[e] = dot(uds[e], wd_buf[slot], 1, 1)

        @pl.when(e + RING < LOC_E)
        def _():
            wd_copy(e + RING).start()

    pl.loop(0, LOC_E // 2)(back_step)
    first_relays(1)
    pl.loop(LOC_E // 2, LOC_E)(back_step)
    second_forwards(1)
    for role in (X_ | P_, Y_ | P_):
        for k in range(2):
            arrived(1, role, k)
    gather(1, 1)
    gather(1, 2)
    last_forwards(1)
    for k in range(2):
        arrived(1, X_ | Y_ | P_, k)
    gather(1, 3)
    xs_copy = pltpu.make_async_copy(xs, xs_ref, out_sem.at[1])
    xs_copy.start()

    pres, hids, dabs = (pre0, pre1), (hid0, hid1), (dab0, dab1)

    def st_copies(e, b):
        return (pltpu.make_async_copy(hids[b], hid_ref.at[e], st_sem.at[b, 0]),
                pltpu.make_async_copy(dabs[b], dab_ref.at[e], st_sem.at[b, 1]))

    def up_step(e, b):
        pres[b][...] = dot(xs[e], w_buf[lax.rem(e, W_RING)])

    def mid_step(e, b):
        pre_gate = pres[b][:, :F]
        pre_up = pres[b][:, F:]
        sig = jax.nn.sigmoid(pre_gate)
        silu = pre_gate * sig
        hidden = (silu * pre_up).astype(BF16)
        d_hidden = back[e, :SLOTS]
        dgs[e] = jnp.broadcast_to(jnp.sum(hidden.astype(F32) * back[e, SLOTS:], axis=1, keepdims=True), (SLOTS, 128))
        hids[b][...] = hidden
        dabs[b][:, :F] = (d_hidden * pre_up * sig * (1.0 + pre_gate * (1.0 - sig))).astype(BF16)
        dabs[b][:, F:] = (d_hidden * silu).astype(BF16)

    def c_step(e, b):
        c = dot(dabs[b][...], w_buf[lax.rem(e, W_RING)], 1, 1).astype(BF16)
        for q in range(N_PAIR):
            cs[q, pl.ds(pl.multiple_of(e * PAIR, 16), PAIR), :] = c[q * PAIR:(q + 1) * PAIR]

    def wait_all(copies):
        for copy in copies:
            copy.wait()

    def start_all(copies):
        for copy in copies:
            copy.start()

    wait_all(w_copies(0))
    wait_all(w_copies(1))
    up_step(0, 0)
    up_step(1, 1)
    mid_step(0, 0)
    start_all(st_copies(0, 0))

    @pl.loop(0, LOC_E // 2 - 1)
    def _(i):
        e = 2 * i + 1
        wait_all(w_copies(e + 1))
        wait_all(w_copies(e + 2))

        @pl.when(i > 0)
        def _():
            wait_all(st_copies(e - 2, 1))

        up_step(e + 1, 0)
        mid_step(e, 1)
        c_step(e - 1, 0)
        start_all(st_copies(e, 1))
        wait_all(st_copies(e - 1, 0))
        up_step(e + 2, 1)
        mid_step(e + 1, 0)
        c_step(e, 1)
        start_all(st_copies(e + 1, 0))

        @pl.when(e + 5 < LOC_E)
        def _():
            start_all(w_copies(e + 5))

        @pl.when(e + 6 < LOC_E)
        def _():
            start_all(w_copies(e + 6))

    wait_all(st_copies(LOC_E - 3, 1))
    mid_step(LOC_E - 1, 1)
    c_step(LOC_E - 2, 0)
    start_all(st_copies(LOC_E - 1, 1))
    c_step(LOC_E - 1, 1)

    dg_copies = []
    for r in range(N_DEV):
        mask = ranks[r][:, None, :] == slot_iota(CAP)
        vals = dgs[:, r * CAP:(r + 1) * CAP, :][:, :, :1]
        dg_out[r] = jnp.sum(jnp.where(mask, vals, 0.0), axis=1)
        if r:
            copy = pltpu.make_async_remote_copy(
                src_ref=dg_out.at[r], dst_ref=dg_in.at[r], send_sem=dg_send.at[r], recv_sem=dg_recv.at[r],
                device_id=role_id(r), device_id_type=MESH)
            copy.start()
            dg_copies.append(copy)

    for copy in sends:
        copy.wait_send()
    part_copies = []
    for r in range(N_DEV):
        q, h = r // 2, r % 2

        wide = (ranks[r] + float(h * CAP))[:, None, :] == slot_iota(PAIR)
        hot = jnp.where(wide, 1.0, 0.0).reshape(PAIR_ROWS, N_TOK).astype(BF16)
        for c in range(4):
            cols = slice(c * 256, (c + 1) * 256)
            xa[r, :, cols] = dot(hot, cs[q, :, cols], 0, 0).astype(BF16)
        g, l = role_coords(r)
        copy = pltpu.make_async_copy(xa.at[r], part_ref.at[l * 4 + g], out_sem.at[2 + r])
        copy.start()
        part_copies.append(copy)

    for copy in dg_copies:
        copy.wait_recv()
    bases = [role_expert_base(r) for r in range(N_DEV)]
    row_iota = lax.broadcasted_iota(jnp.int32, (LOC_E, N_TOK), 0)
    for j in range(TOP_K):
        want = ids_all[0, j:j + 1, :]
        acc = jnp.zeros((LOC_E, N_TOK), F32)
        for r in range(N_DEV):
            acc = jnp.where(want == row_iota + bases[r], dg_in[r] if r else dg_out[0], acc)
        dgate_ref[pl.ds(j, 1), :] = jnp.sum(acc, axis=0, keepdims=True)

    wait_all(st_copies(LOC_E - 2, 0))
    wait_all(st_copies(LOC_E - 1, 1))
    for copy in [us_copy, xs_copy] + part_copies:
        copy.wait()
    for copy in metas + dg_copies:
        copy.wait_send()


def front(x_rows, dy_rows, ids_t, gates_t, w_gate, w_up, w_down):
    dma = pltpu.SemaphoreType.DMA
    return pl.pallas_call(
        front_kernel,
        out_shape=[jax.ShapeDtypeStruct((N_DEV, N_TOK, D), BF16), jax.ShapeDtypeStruct((TOP_K, N_TOK), F32),
                   jax.ShapeDtypeStruct((LOC_E, SLOTS, D), BF16), jax.ShapeDtypeStruct((LOC_E, SLOTS, D), BF16),
                   jax.ShapeDtypeStruct((LOC_E, SLOTS, F), BF16), jax.ShapeDtypeStruct((LOC_E, SLOTS, 2 * F), BF16)],
        in_specs=[ANY] * 7, out_specs=[ANY, VMEM] + [ANY] * 4,
        scratch_shapes=[
            pltpu.VMEM((N_DEV, N_TOK, D), BF16), pltpu.VMEM((N_DEV, N_TOK, D), BF16), pltpu.VMEM((N_DEV, TOP_K, N_TOK), jnp.int32), pltpu.VMEM((N_DEV, TOP_K, N_TOK), F32),
            pltpu.VMEM((LOC_E, SLOTS, D), BF16), pltpu.VMEM((LOC_E, 2 * SLOTS, D), BF16), pltpu.VMEM((N_PAIR, PAIR_ROWS, D), BF16),
            pltpu.VMEM((N_DEV, LOC_E * CAP, N_TOK), BF16), pltpu.VMEM((N_DEV, LOC_E, CAP, 128), F32), pltpu.VMEM((N_DEV, LOC_E, N_TOK), F32),
            pltpu.VMEM((LOC_E, 2 * SLOTS, F), F32), pltpu.VMEM((LOC_E, SLOTS, 128), F32),
            pltpu.VMEM((RING, F, D), BF16), pltpu.VMEM((W_RING, D, 2 * F), BF16), pltpu.VMEM((SLOTS, 2 * F), F32), pltpu.VMEM((SLOTS, 2 * F), F32),
            pltpu.VMEM((SLOTS, F), BF16), pltpu.VMEM((SLOTS, F), BF16), pltpu.VMEM((SLOTS, 2 * F), BF16), pltpu.VMEM((SLOTS, 2 * F), BF16),
            pltpu.VMEM((N_DEV, LOC_E, N_TOK), F32), pltpu.VMEM((N_DEV, LOC_E, N_TOK), F32),
            dma((40,)), dma((2, N_DEV, 2)), dma((N_DEV,)), dma((N_DEV,)), dma((N_DEV,)), dma((N_DEV,)), dma((N_DEV,)), dma((N_DEV,)), dma((4,)),
            dma((RING,)), dma((W_RING, 2)), dma((2, 2)), dma((2 + N_DEV,))],
        compiler_params=pltpu.CompilerParams(collective_id=0, has_side_effects=True, vmem_limit_bytes=63 * 1024 * 1024),
        name='front',
    )(x_rows, dy_rows, ids_t, gates_t, w_gate, w_up, w_down)


def wgrad_kernel(x_ref, u_ref, hid_ref, dab_ref, dwg_ref, dwu_ref, dwd_ref):
    dwd_ref[0] = dot(hid_ref[0], u_ref[0], 0, 0).astype(BF16)
    both = dot(x_ref[0], dab_ref[0], 0, 0).astype(BF16)
    dwg_ref[0] = both[:, :F]
    dwu_ref[0] = both[:, F:]


def wgrad(xs, us, hid, dab):
    each = lambda *shape: pl.BlockSpec((1,) + shape, lambda e: (e, 0, 0))
    return pl.pallas_call(
        wgrad_kernel,
        grid=(LOC_E,),
        out_shape=[jax.ShapeDtypeStruct((LOC_E, D, F), BF16), jax.ShapeDtypeStruct((LOC_E, D, F), BF16), jax.ShapeDtypeStruct((LOC_E, F, D), BF16)],
        in_specs=[each(SLOTS, D), each(SLOTS, D), each(SLOTS, F), each(SLOTS, 2 * F)],
        out_specs=[each(D, F), each(D, F), each(F, D)],
        compiler_params=pltpu.CompilerParams(vmem_limit_bytes=60 * 1024 * 1024, dimension_semantics=('arbitrary',)),
        cost_estimate=pl.CostEstimate(flops=2 * LOC_E * SLOTS * D * F * 3, bytes_accessed=57_000_000, transcendentals=0),
        name='wgrad',
    )(xs, us, hid, dab)


def final_kernel(parts_ref, dx_ref):
    @pl.loop(0, N_TOK // 16)
    def _(i):
        rows = pl.ds(pl.multiple_of(i * 16, 16), 16)
        total = jnp.zeros((16, D), F32)
        for g in range(4):
            total += (parts_ref[g, rows].astype(F32) + parts_ref[4 + g, rows].astype(F32)).astype(BF16).astype(F32)
        dx_ref[rows] = total.astype(BF16)


def final_sum(parts):
    return pl.pallas_call(
        final_kernel,
        out_shape=jax.ShapeDtypeStruct((N_TOK, D), BF16),
        in_specs=[VMEM],
        out_specs=VMEM,
        compiler_params=pltpu.CompilerParams(vmem_limit_bytes=16 * 1024 * 1024),
        name='final_sum',
    )(parts)


def solution(mesh):
    spec = P(('part', 'grp', 'loc'))

    def device_step(x_rows, dy_rows, expert_ids, gate_vals, w_gate, w_up, w_down):
        part, dgate_t, xs, us, hid, dab = front(x_rows, dy_rows, expert_ids.T, gate_vals.T, w_gate, w_up, w_down)
        parts = lax.all_to_all(part, ('loc', 'grp'), 0, 0)
        dwg, dwu, dwd = wgrad(xs, us, hid, dab)
        return final_sum(parts), dgate_t.T, dwg, dwu, dwd

    return jax.shard_map(device_step, mesh=mesh, in_specs=(spec,) * 7, out_specs=(spec,) * 5, check_vma=False)
```
